32 devices in a mesh: data: 4 (over x, y), seq: 8 (over z, core).
Axes of the slice: x: 2, y: 2, z: 4, core: 2. Of those that a mesh axis runs over, the one named last changes fastest.
Arguments:
- x_in: bfloat16 [3, 4096, 4096], P(None, ('data', 'seq')), parts along dimension 1
- positions: int32 [4096], P(('data', 'seq')), parts along dimension 0
- w_query: bfloat16 [3, 4096, 32, 128], replicated
- w_key: bfloat16 [3, 4096, 32, 128], replicated
- w_value: bfloat16 [3, 4096, 32, 128], replicated
- w_out: bfloat16 [3, 32, 128, 4096], replicated
- w_up: bfloat16 [3, 4096, 11008], replicated
- w_down: bfloat16 [3, 11008, 4096], replicated
- g_attn: float32 [3, 4096], replicated
- g_mlp: float32 [3, 4096], replicated
Outputs:
- output: bfloat16 [3, 4096, 4096], P(None, ('data', 'seq')), parts along dimension 1
There are 4 independent parts. The reference program is written for one: setup_inputs(seed, part) draws one part's arguments, and reference() takes and returns one part's arrays. A program takes and returns all parts, laid end to end along the dimension named above; an argument that names none is the same for every part.
All inputs are finite; a program needn't handle non-finite values.
Results may differ from the reference program's by a relative error of at most 0.0164023.
Values are sent between devices in bfloat16 or wider.
A program may use at most 3.75 GiB of HBM per device.

```python
import jax
import jax.numpy as jnp
from jax import lax

BATCH_SIZE = 3
SEQ_LEN = 1024
D_MODEL = 4096
N_HEADS = 32
N_KV_HEADS = 32
HEAD_DIM = 128
FF_DIM = 11008
N_LAYERS = 3
REF_BLOCK = 64

ROPE_BASE = 10000.0
NORM_EPS = 1e-6


def normal_weights(rng_key, w_shape, fan_in, w_gain):
    return (jax.random.normal(rng_key, w_shape, jnp.float32) * (w_gain * fan_in ** -0.5)).astype(jnp.bfloat16)


def setup_inputs(seed: int = 0, part: int = 0) -> dict:
    base_key = jax.random.key(seed)
    part_keys = jax.random.split(jax.random.fold_in(base_key, part), 6)
    weight_keys = jax.random.split(jax.random.fold_in(base_key, 100003), 8)
    step_frac = jnp.arange(SEQ_LEN, dtype=jnp.float32) / SEQ_LEN
    wave_freq = jax.random.uniform(part_keys[0], (BATCH_SIZE, 4), jnp.float32, minval=0.5, maxval=3.0)
    wave_phase = jax.random.uniform(part_keys[1], (BATCH_SIZE, 4), jnp.float32, minval=0.0, maxval=6.283185)
    wave_vals = jnp.cos(6.283185 * wave_freq[:, :, None] * step_frac[None, None, :] + wave_phase[:, :, None])
    wave_dirs = jax.random.normal(part_keys[2], (BATCH_SIZE, 4, D_MODEL), jnp.float32)
    smooth = jnp.einsum("bjs,bjd->bsd", wave_vals, wave_dirs) * 0.5
    noise_part = jax.random.normal(part_keys[3], (BATCH_SIZE, SEQ_LEN, D_MODEL), jnp.float32) * 0.7
    offset = jax.random.randint(part_keys[4], (), 0, SEQ_LEN)
    pos_gaps = jax.random.randint(part_keys[5], (SEQ_LEN,), 1, 5)
    return {
        "x_in": (smooth + noise_part).astype(jnp.bfloat16),
        "positions": (offset + jnp.cumsum(pos_gaps)).astype(jnp.int32),
        "w_query": normal_weights(weight_keys[0], (N_LAYERS, D_MODEL, N_HEADS, HEAD_DIM), D_MODEL, 1.25),
        "w_key": normal_weights(weight_keys[1], (N_LAYERS, D_MODEL, N_KV_HEADS, HEAD_DIM), D_MODEL, 1.25),
        "w_value": normal_weights(weight_keys[2], (N_LAYERS, D_MODEL, N_KV_HEADS, HEAD_DIM), D_MODEL, 1.0),
        "w_out": normal_weights(weight_keys[3], (N_LAYERS, N_HEADS, HEAD_DIM, D_MODEL), N_HEADS * HEAD_DIM, 1.0),
        "w_up": normal_weights(weight_keys[4], (N_LAYERS, D_MODEL, FF_DIM), D_MODEL, 1.0),
        "w_down": normal_weights(weight_keys[5], (N_LAYERS, FF_DIM, D_MODEL), FF_DIM, 1.0),
        "g_attn": jax.random.uniform(weight_keys[6], (N_LAYERS, D_MODEL), jnp.float32, minval=0.5, maxval=1.5),
        "g_mlp": jax.random.uniform(weight_keys[7], (N_LAYERS, D_MODEL), jnp.float32, minval=0.5, maxval=1.5),
    }


def rms_norm(x_act, gain_vec):
    x_f32 = x_act.astype(jnp.float32)
    mean_sq = jnp.mean(x_f32 * x_f32, axis=-1, keepdims=True)
    return (x_f32 * lax.rsqrt(mean_sq + NORM_EPS) * gain_vec).astype(jnp.bfloat16)


def rope_tables(positions):
    inv_freq = ROPE_BASE ** (-jnp.arange(HEAD_DIM // 2, dtype=jnp.float32) * (2.0 / HEAD_DIM))
    angles = positions.astype(jnp.float32)[:, None] * inv_freq[None, :]
    return jnp.cos(angles), jnp.sin(angles)


def apply_rope(proj_f32, cos_t, sin_t):
    half_dim = HEAD_DIM // 2
    x_first = proj_f32[..., :half_dim]
    x_second = proj_f32[..., half_dim:]
    cos_b = cos_t[:, None, :]
    sin_b = sin_t[:, None, :]
    return jnp.concatenate([x_first * cos_b - x_second * sin_b, x_second * cos_b + x_first * sin_b], axis=-1).astype(jnp.bfloat16)


def causal_attention(q_heads, k_heads, v_heads):
    groups = N_HEADS // N_KV_HEADS
    n_blocks = SEQ_LEN // REF_BLOCK
    att_scale = HEAD_DIM ** -0.5
    q_grouped = q_heads.reshape(BATCH_SIZE, SEQ_LEN, N_KV_HEADS, groups, HEAD_DIM)
    k_f32 = k_heads.astype(jnp.float32)
    v_f32 = v_heads.astype(jnp.float32)
    key_pos = jnp.arange(SEQ_LEN)

    def one_block(blk_idx):
        blk_start = blk_idx * REF_BLOCK
        q_blk = lax.dynamic_slice_in_dim(q_grouped, blk_start, REF_BLOCK, axis=1).astype(jnp.float32)
        scores = jnp.einsum("bqkgd,bskd->bkgqs", q_blk, k_f32) * att_scale
        query_pos = blk_start + jnp.arange(REF_BLOCK)
        allowed = key_pos[None, :] <= query_pos[:, None]
        scores = jnp.where(allowed, scores, -1e30)
        row_max = jnp.max(scores, axis=-1, keepdims=True)
        exp_f32 = jnp.exp(scores - row_max)
        row_sum = jnp.sum(exp_f32, axis=-1)
        weighted = jnp.einsum("bkgqs,bskd->bqkgd", exp_f32.astype(jnp.bfloat16).astype(jnp.float32), v_f32)
        return (weighted / jnp.transpose(row_sum, (0, 3, 1, 2))[..., None]).astype(jnp.bfloat16)

    blocks = lax.map(one_block, jnp.arange(n_blocks))
    return jnp.moveaxis(blocks, 0, 1).reshape(BATCH_SIZE, SEQ_LEN, N_HEADS, HEAD_DIM)


def transformer_layer(hidden, cos_t, sin_t, layer_weights):
    w_query, w_key, w_value, w_out, w_up, w_down, gain_attn, gain_mlp = layer_weights
    n_rows = BATCH_SIZE * SEQ_LEN
    normed = rms_norm(hidden, gain_attn).reshape(n_rows, D_MODEL)
    q_proj = jnp.dot(normed, w_query.reshape(D_MODEL, N_HEADS * HEAD_DIM), preferred_element_type=jnp.float32)
    k_proj = jnp.dot(normed, w_key.reshape(D_MODEL, N_KV_HEADS * HEAD_DIM), preferred_element_type=jnp.float32)
    v_proj = jnp.dot(normed, w_value.reshape(D_MODEL, N_KV_HEADS * HEAD_DIM), preferred_element_type=jnp.float32)
    q_heads = apply_rope(q_proj.reshape(BATCH_SIZE, SEQ_LEN, N_HEADS, HEAD_DIM), cos_t, sin_t)
    k_heads = apply_rope(k_proj.reshape(BATCH_SIZE, SEQ_LEN, N_KV_HEADS, HEAD_DIM), cos_t, sin_t)
    v_heads = v_proj.astype(jnp.bfloat16).reshape(BATCH_SIZE, SEQ_LEN, N_KV_HEADS, HEAD_DIM)
    attn_out = causal_attention(q_heads, k_heads, v_heads)
    attn_proj = jnp.dot(attn_out.reshape(n_rows, N_HEADS * HEAD_DIM), w_out.reshape(N_HEADS * HEAD_DIM, D_MODEL), preferred_element_type=jnp.float32)
    resid_h = (hidden.reshape(n_rows, D_MODEL).astype(jnp.float32) + attn_proj).astype(jnp.bfloat16)
    normed_mlp = rms_norm(resid_h, gain_mlp)
    gelu_act = jax.nn.gelu(jnp.dot(normed_mlp, w_up, preferred_element_type=jnp.float32), approximate=True).astype(jnp.bfloat16)
    layer_out = resid_h.astype(jnp.float32) + jnp.dot(gelu_act, w_down, preferred_element_type=jnp.float32)
    return layer_out.astype(jnp.bfloat16).reshape(BATCH_SIZE, SEQ_LEN, D_MODEL)


def reference(x_in, positions, w_query, w_key, w_value, w_out, w_up, w_down, g_attn, g_mlp):
    cos_t, sin_t = rope_tables(positions)

    def layer_body(hidden, layer_weights):
        return transformer_layer(hidden, cos_t, sin_t, layer_weights), None

    stacked = (w_query, w_key, w_value, w_out, w_up, w_down, g_attn, g_mlp)
    return lax.scan(layer_body, x_in, stacked)[0]
```

```python
import functools

import jax
import jax.numpy as jnp
from jax import lax
from jax.experimental import pallas as pl
from jax.experimental.pallas import tpu as pltpu
from jax.sharding import PartitionSpec as P

ROPE_BASE = 10000.0
NORM_EPS = 1e-6
NEG = -1e30
LOG2E = 1.4426950408889634
F32 = jnp.float32
BF16 = jnp.bfloat16
MESH = pl.DeviceIdType.MESH

ROUTE = (
    ((0, 0), (1, 1), (2, 0)),
    ((1, 0), (1, 2), (3, 0)),
    ((0, 1), (2, 1), (3, 1)),
    ((0, 2), (2, 2), (3, 2)),
)
SEND_ORDER = ((1, 2), (2,), (0, 2), (1, 0))
HOME = tuple(
    tuple(next((i, q) for i in range(4) for q in range(3) if ROUTE[i][q] == (c, s)) for s in range(3))
    for c in range(4)
)
KV_SENDS = (((0, 1, 0),), ((1, 2, 0), (2, 2, 1), (0, 0, 0)), ((0, 3, 0),), ())

ROWS = 128
TOK = 3 * ROWS
TN = 1024
HG = 8


def dot(a, b):
    return jnp.dot(a, b, preferred_element_type=F32)


def gelu_tanh(x):
    c0 = 0.7978845608028654
    t = jnp.tanh(x * (c0 + (c0 * 0.044715) * (x * x)))
    h = 0.5 * x
    return h + h * t


def layers_kernel(
    n_layers, d_model, ff,
    x_ref, tab_ref, ga_ref, gm_ref, wq_ref, wk_ref, wv_ref, wo_ref, wu_ref, wd_ref,
    y_ref,
    hbuf, nbuf, pbuf, rbuf, obuf, acc, mask, ring, qring,
    wsem, qsem, xs_sem, xr_sem, ns_sem, nr_sem, ks_sem, kr_sem, os_sem, or_sem, ys_sem, yr_sem, cred,
):
    me = lax.axis_index("seq")
    core = lax.rem(me, 2)
    chip = me // 2
    partner = {"seq": me + 1 - 2 * core}

    n_out = d_model // TN
    n_up = -(-ff // TN)
    tail = ff - (n_up - 1) * TN
    k_units = ff // 256
    cuts = [0, (k_units // 3) * 256, 2 * (k_units // 3) * 256, ff]
    tiles = n_out + n_up + 3 * n_out
    o_rows = 4 * TN

    def on_chip(c):
        return {"seq": 2 * c + core}

    def cols(i):
        return pl.ds(pl.multiple_of(i * TN, TN), TN)

    def q_copy(l, i):
        w = (wk_ref, wv_ref)
        return w, l, i

    def q_start(l, i):
        for kind, ref in enumerate((wk_ref, wv_ref, wq_ref)):
            for g in range(2):
                idx = 2 * g + kind if kind < 2 else 4 + g

                @pl.when(i == idx)
                def _(ref=ref, g=g, idx=idx):
                    heads = pl.ds(pl.multiple_of(core * 2 * HG + g * HG, HG), HG)
                    pltpu.make_async_copy(ref.at[l, :, heads, :], qring.at[idx % 2], qsem.at[idx % 2]).start()

    def q_wait(slot):
        pltpu.make_async_copy(wq_ref.at[0, :, pl.ds(0, HG), :], qring.at[slot], qsem.at[slot]).wait()

    def t_slot(l, t):
        return lax.rem(l * tiles + t, 2)

    def out_copy(l, i):
        s = t_slot(l, i)
        return pltpu.make_async_copy(wo_ref.at[l, :, cols(i)], ring.at[s, pl.ds(0, o_rows)], wsem.at[s])

    def up_copy(l, i):
        s = t_slot(l, n_out + i)
        return pltpu.make_async_copy(wu_ref.at[l, :, cols(i)], ring.at[s, pl.ds(0, d_model)], wsem.at[s])

    def up_tail_copy(l):
        s = t_slot(l, n_out + n_up - 1)
        src = wu_ref.at[l, :, pl.ds((n_up - 1) * TN, tail)]
        return pltpu.make_async_copy(src, ring.at[s, pl.ds(0, d_model), pl.ds(0, tail)], wsem.at[s])

    def down_copy(l, n, kk):
        s = t_slot(l, n_out + n_up + 3 * n + kk)
        size = cuts[kk + 1] - cuts[kk]
        return pltpu.make_async_copy(
            wd_ref.at[l, pl.ds(cuts[kk], size), cols(n)], ring.at[s, pl.ds(0, size)], wsem.at[s])

    q_start(0, 0)
    out_copy(0, 0).start()

    barrier = pltpu.get_barrier_semaphore()
    for k in range(1, 8):
        pl.semaphore_signal(barrier, inc=1, device_id={"seq": lax.rem(me + k, 8)}, device_id_type=MESH)
    pl.semaphore_wait(barrier, 7)

    def rows(t):
        return pl.ds(t * ROWS, ROWS)

    for c in range(4):
        @pl.when(chip == c)
        def _(c=c):
            for k, q in enumerate(SEND_ORDER[c]):
                dst, slot = ROUTE[c][q]
                pltpu.make_async_remote_copy(
                    src_ref=x_ref.at[q], dst_ref=hbuf.at[rows(slot)], send_sem=xs_sem.at[k],
                    recv_sem=xr_sem.at[slot], device_id=on_chip(dst), device_id_type=MESH).start()
            for q in range(3):
                dst, slot = ROUTE[c][q]
                if dst == c:
                    pltpu.make_async_copy(x_ref.at[q], hbuf.at[rows(slot)], xr_sem.at[slot]).start()

    ri = lax.broadcasted_iota(jnp.int32, (2 * ROWS, 2 * ROWS), 0)
    ci = lax.broadcasted_iota(jnp.int32, (2 * ROWS, 2 * ROWS), 1)
    flip = core * ROWS
    rp = jnp.where(ri < ROWS, ri + flip, ri - flip)
    cp = jnp.where(ci < ROWS, ci + flip, ci - flip)
    mask[...] = jnp.where(cp <= rp, 0.0, NEG)

    def norm_rows(gain, t):
        def step(i, _):
            r = pl.ds(pl.multiple_of(t * ROWS + i * 16, 16), 16)
            v = hbuf[r, :].astype(F32)
            scale = lax.rsqrt(jnp.mean(v * v, axis=1, keepdims=True) + NORM_EPS)
            nbuf[0, r, :] = (v * scale * gain).astype(BF16)
            return 0

        lax.fori_loop(0, ROWS // 16, step, 0)

    def n_send(t):
        return pltpu.make_async_remote_copy(
            src_ref=nbuf.at[0, rows(t)], dst_ref=nbuf.at[1, rows(t)], send_sem=ns_sem.at[t],
            recv_sem=nr_sem.at[t], device_id=partner, device_id_type=MESH)

    def kv_send(i, s, k, slot, dst, rslot):
        base = 4 + 4 * (i % 2) + 2 * (i // 2) if isinstance(i, int) else 4 + 4 * lax.rem(i, 2) + 2 * (i // 2)
        return pltpu.make_async_remote_copy(
            src_ref=pbuf.at[base + s, rows(slot)], dst_ref=rbuf.at[i, rslot, s], send_sem=ks_sem.at[i, s, k],
            recv_sem=kr_sem.at[i, rslot, s], device_id=on_chip(dst), device_id_type=MESH)

    def kv_wait(i, s, rslot):
        pltpu.make_async_remote_copy(
            src_ref=pbuf.at[0, rows(0)], dst_ref=rbuf.at[i, rslot, s], send_sem=ks_sem.at[i, s, 0],
            recv_sem=kr_sem.at[i, rslot, s], device_id=partner, device_id_type=MESH).wait_recv()

    def o_send(g):
        piece = core * 2 + g
        return pltpu.make_async_remote_copy(
            src_ref=pbuf.at[2 * g + 1], dst_ref=obuf.at[piece], send_sem=os_sem.at[g],
            recv_sem=or_sem.at[g], device_id=partner, device_id_type=MESH)

    def layer(l, _):
        gain = ga_ref[l]
        for t in range(3):
            @pl.when(l == 0)
            def _(t=t):
                pltpu.make_async_copy(x_ref.at[0], hbuf.at[rows(t)], xr_sem.at[t]).wait()

            norm_rows(gain, t)
            if t > 0:
                n_send(t - 1).start()

        def qkv_tile(i, _):
            slot = lax.rem(i, 2)
            q_wait(slot)

            @pl.when(i < 5)
            def _():
                q_start(l, i + 1)

            @pl.when(jnp.logical_and(i == 5, l < n_layers - 1))
            def _():
                q_start(l + 1, 0)

            def side(s, _):
                b = 2 * i + s

                @pl.when(b == 0)
                def _():
                    n_send(2).start()

                @pl.when(b == 1)
                def _():
                    for t in range(3):
                        n_send(t).wait_recv()

                    @pl.when(l > 0)
                    def _():
                        for c in range(4):
                            @pl.when(chip == c)
                            def _(c=c):
                                for k in sorted({1 if dst == 2 else 0 for _, dst, _ in KV_SENDS[c]}):
                                    pl.semaphore_wait(cred.at[k], 1)

                @pl.when(jnp.logical_and(b >= 1, b <= 8))
                def _():
                    pi = (b - 1) // 2
                    ps = lax.rem(b - 1, 2)
                    for c in range(4):
                        @pl.when(chip == c)
                        def _(c=c):
                            for k, (sl, dst, rs) in enumerate(KV_SENDS[c]):
                                kv_send(pi, ps, k, sl, dst, rs).start()

                kq = d_model // 8
                u = functools.reduce(jnp.add, [
                    dot(nbuf[s, :, j * kq:(j + 1) * kq], qring[slot, j * kq:(j + 1) * kq].reshape(kq, TN))
                    for j in range(8)])
                piece = jnp.where(i < 4, 4 + 4 * lax.rem(i, 2) + 2 * (i // 2), 2 * (i - 4)) + s
                plain = jnp.logical_and(lax.rem(i, 2) == 1, i < 4)
                cos = jnp.where(plain, 1.0, tab_ref[0, s])
                sin = jnp.where(plain, 0.0, tab_ref[1, s])
                for h in range(HG):
                    uh = u[:, h * 128:(h + 1) * 128]
                    pbuf[piece, :, h * 128:(h + 1) * 128] = (
                        uh * cos + pltpu.roll(uh, 64, axis=1) * sin).astype(BF16)

                @pl.when(jnp.logical_and(i < 4, chip != 2))
                def _():
                    rbuf[jnp.minimum(i, 3), 1, s] = pbuf[piece, 0:ROWS, :]

                return 0

            lax.fori_loop(0, 2, side, 0)
            return 0

        lax.fori_loop(0, 6, qkv_tile, 0)
        for t in range(3):
            n_send(t).wait_send()

        bias0 = jnp.where(lax.rem(chip, 2) == 1, 0.0, NEG)
        bias1 = jnp.where(chip == 1, NEG, 0.0)
        c2 = 128 ** -0.5 * LOG2E

        def group(g, _):
            for j in range(2):
                for s in range(2):
                    kv_wait(2 * g + j, s, 0)

            @pl.when(chip == 2)
            def _():
                for j in range(2):
                    for s in range(2):
                        kv_wait(2 * g + j, s, 1)

            @pl.when(g == 1)
            def _():
                o_send(0).start()

            def head(h, _):
                lanes = pl.ds(pl.multiple_of(h * 128, 128), 128)

                def local(base, t):
                    r = rows(t)
                    return jnp.concatenate([pbuf[base + 2 * g, r, lanes], pbuf[base + 2 * g + 1, r, lanes]], axis=0)

                def remote(j, rs):
                    return jnp.concatenate([rbuf[2 * g + j, rs, 0, :, lanes], rbuf[2 * g + j, rs, 1, :, lanes]], axis=0)

                for t in range(3):
                    q = local(0, t)
                    blocks = [(remote(0, 0), remote(1, 0), bias0 if t == 0 else bias1)]
                    if t > 0:
                        blocks.append((remote(0, 1), remote(1, 1), bias1))
                    if t == 2:
                        blocks.append((local(4, 1), local(8, 1), None))
                    blocks.append((local(4, t), local(8, t), mask[...]))
                    xs = []
                    for k, _, b in blocks:
                        sc = lax.dot_general(q, k, (((1,), (1,)), ((), ())), preferred_element_type=F32) * c2
                        xs.append(sc if b is None else sc + b)
                    top = functools.reduce(jnp.maximum, xs)
                    top = jnp.max(top, axis=1, keepdims=True)
                    es = [jnp.exp2(v - top) for v in xs]
                    total = jnp.sum(functools.reduce(jnp.add, es), axis=1, keepdims=True)
                    o = functools.reduce(jnp.add, [dot(e.astype(BF16), v) for e, (_, v, _) in zip(es, blocks)])
                    o = (o * (1.0 / total)).astype(BF16)
                    obuf[core * 2 + g, rows(t), lanes] = o[:ROWS]
                    pbuf[2 * g + 1, rows(t), lanes] = o[ROWS:]
                return 0

            lax.fori_loop(0, HG, head, 0)
            return 0

        lax.fori_loop(0, 2, group, 0)

        for c in range(4):
            @pl.when(chip == c)
            def _(c=c):
                for i in range(4):
                    for s in range(2):
                        for k, (sl, dst, rs) in enumerate(KV_SENDS[c]):
                            kv_send(i, s, k, sl, dst, rs).wait_send()

                @pl.when(l < n_layers - 1)
                def _():
                    src, k = ((1, 0), (0, 0), (1, 1), (2, 0))[c]
                    pl.semaphore_signal(cred.at[k], inc=1, device_id=on_chip(src), device_id_type=MESH)

        o_send(1).start()
        for g in range(2):
            o_send(g).wait_recv()

        def out_tile(i, _):
            out_copy(l, i).wait()

            @pl.when(i < n_out - 1)
            def _():
                out_copy(l, i + 1).start()

            @pl.when(i == n_out - 1)
            def _():
                up_copy(l, 0).start()

            slot = t_slot(l, i)
            u = functools.reduce(
                jnp.add, [dot(obuf[j], ring[slot, j * TN:(j + 1) * TN, :]) for j in range(4)])
            hbuf[:, cols(i)] = (hbuf[:, cols(i)].astype(F32) + u).astype(BF16)
            return 0

        lax.fori_loop(0, n_out, out_tile, 0)
        for g in range(2):
            o_send(g).wait_send()

        gain_m = gm_ref[l]
        for t in range(3):
            norm_rows(gain_m, t)

        def up_tile(i, _):
            @pl.when(i < n_up - 1)
            def _():
                up_copy(l, i).wait()

            @pl.when(i == n_up - 1)
            def _():
                up_tail_copy(l).wait()

            @pl.when(i < n_up - 2)
            def _():
                up_copy(l, i + 1).start()

            @pl.when(i == n_up - 2)
            def _():
                up_tail_copy(l).start()

            @pl.when(i == n_up - 1)
            def _():
                down_copy(l, 0, 0).start()

            slot = t_slot(l, n_out + i)
            pbuf[i] = gelu_tanh(dot(nbuf[0], ring[slot, 0:d_model, :])).astype(BF16)
            return 0

        lax.fori_loop(0, n_up, up_tile, 0)

        def y_send(c, t, n):
            dst, q = HOME[c][t]
            if dst == c:
                return pltpu.make_async_copy(hbuf.at[rows(t), cols(n)], y_ref.at[q, :, cols(n)], yr_sem.at[q, n])
            return pltpu.make_async_remote_copy(
                src_ref=hbuf.at[rows(t), cols(n)], dst_ref=y_ref.at[q, :, cols(n)], send_sem=ys_sem.at[t, n],
                recv_sem=yr_sem.at[q, n], device_id=on_chip(dst), device_id_type=MESH)

        def y_start(n):
            for c in range(4):
                @pl.when(chip == c)
                def _(c=c):
                    for t in range(3):
                        y_send(c, t, n).start()

        def down_tile(n, _):
            for kk in range(3):
                down_copy(l, n, kk).wait()
                if kk < 2:
                    down_copy(l, n, kk + 1).start()
                else:
                    @pl.when(n < n_out - 1)
                    def _():
                        down_copy(l, n + 1, 0).start()

                    @pl.when(jnp.logical_and(n == n_out - 1, l < n_layers - 1))
                    def _():
                        out_copy(l + 1, 0).start()

                if kk == 0:
                    @pl.when(jnp.logical_and(n > 0, l == n_layers - 1))
                    def _():
                        y_start(n - 1)

                slot = t_slot(l, n_out + n_up + 3 * n + kk)
                parts = []
                lo = cuts[kk]
                while lo < cuts[kk + 1]:
                    hi = min((lo // TN + 1) * TN, cuts[kk + 1])
                    parts.append(dot(pbuf[lo // TN, :, lo % TN:lo % TN + hi - lo],
                                     ring[slot, lo - cuts[kk]:hi - cuts[kk], :]))
                    lo = hi
                u = functools.reduce(jnp.add, parts)
                if kk == 0:
                    acc[...] = u
                elif kk == 1:
                    acc[...] += u
                else:
                    hbuf[:, cols(n)] = (hbuf[:, cols(n)].astype(F32) + (acc[...] + u)).astype(BF16)
            return 0

        lax.fori_loop(0, n_out, down_tile, 0)

        @pl.when(l == n_layers - 1)
        def _():
            for c in range(4):
                @pl.when(chip == c)
                def _(c=c):
                    for k, q in enumerate(SEND_ORDER[c]):
                        dst, slot = ROUTE[c][q]
                        pltpu.make_async_remote_copy(
                            src_ref=x_ref.at[q], dst_ref=hbuf.at[rows(slot)], send_sem=xs_sem.at[k],
                            recv_sem=xr_sem.at[slot], device_id=on_chip(dst), device_id_type=MESH).wait_send()
            y_start(n_out - 1)
            for c in range(4):
                @pl.when(chip == c)
                def _(c=c):
                    for n in range(n_out):
                        for t in range(3):
                            if HOME[c][t][0] != c:
                                y_send(c, t, n).wait_send()
            for n in range(n_out):
                for q in range(3):
                    pltpu.make_async_copy(hbuf.at[rows(0), cols(n)], y_ref.at[q, :, cols(n)], yr_sem.at[q, n]).wait()

        return 0

    lax.fori_loop(0, n_layers, layer, 0)


def run_layers(x_loc, tab, g_attn, g_mlp, w_query, w_key, w_value, w_out, w_up, w_down):
    n_layers, d_model = g_attn.shape
    ff = w_up.shape[-1]
    n_out = d_model // TN
    k_units = ff // 256
    ring_rows = max(4 * TN, d_model, (k_units - 2 * (k_units // 3)) * 256)
    vmem = pl.BlockSpec(memory_space=pltpu.VMEM)
    hbm = pl.BlockSpec(memory_space=pl.ANY)
    dma = pltpu.SemaphoreType.DMA
    n_pieces = max(12, -(-ff // TN))
    return pl.pallas_call(
        functools.partial(layers_kernel, n_layers, d_model, ff),
        out_shape=jax.ShapeDtypeStruct(x_loc.shape, BF16),
        in_specs=[hbm, vmem, vmem, vmem] + [hbm] * 6,
        out_specs=hbm,
        scratch_shapes=[
            pltpu.VMEM((TOK, d_model), BF16),
            pltpu.VMEM((2, TOK, d_model), BF16),
            pltpu.VMEM((n_pieces, TOK, TN), BF16),
            pltpu.VMEM((4, 2, 2, ROWS, TN), BF16),
            pltpu.VMEM((4, TOK, TN), BF16),
            pltpu.VMEM((TOK, TN), F32),
            pltpu.VMEM((2 * ROWS, 2 * ROWS), F32),
            pltpu.VMEM((2, ring_rows, TN), BF16),
            pltpu.VMEM((2, d_model, HG, 128), BF16),
            dma((2,)), dma((2,)), dma((2,)), dma((3,)), dma((3,)), dma((3,)),
            dma((4, 2, 3)), dma((4, 2, 2)), dma((2,)), dma((2,)), dma((3, n_out)), dma((3, n_out)),
            pltpu.SemaphoreType.REGULAR((2,)),
        ],
        compiler_params=pltpu.CompilerParams(
            collective_id=0, has_side_effects=True, vmem_limit_bytes=67043328),
        name="layers",
    )(x_loc, tab, g_attn.reshape(n_layers, 1, d_model), g_mlp.reshape(n_layers, 1, d_model),
      w_query, w_key, w_value, w_out.reshape(n_layers, -1, d_model), w_up, w_down)


def rope_tables(pos_loc):
    me = lax.axis_index("seq")
    core, chip = me % 2, me // 2
    pos_all = lax.all_gather(pos_loc, "seq")
    home = jnp.array([[HOME[c][s][0] for s in range(3)] for c in range(4)], jnp.int32)
    chunk = lax.dynamic_index_in_dim(home, chip, 0, keepdims=False)
    side = jnp.stack([core, 1 - core])
    pos = pos_all[(2 * chunk[None, :] + side[:, None])].reshape(2, TOK)
    inv_freq = ROPE_BASE ** (-jnp.arange(64, dtype=F32) * (2.0 / 128))
    angles = pos.astype(F32)[..., None] * inv_freq
    cos, sin = jnp.cos(angles), jnp.sin(angles)
    return jnp.stack([jnp.concatenate([cos, cos], -1), jnp.concatenate([-sin, sin], -1)])


def solution(mesh):
    tok_spec = P(None, ("data", "seq"), None)
    in_specs = (tok_spec, P(("data", "seq"))) + (P(),) * 8

    def device_fn(x_loc, pos_loc, w_query, w_key, w_value, w_out, w_up, w_down, g_attn, g_mlp):
        tab = rope_tables(pos_loc)
        return run_layers(x_loc, tab, g_attn, g_mlp, w_query, w_key, w_value, w_out, w_up, w_down)

    return jax.shard_map(device_fn, mesh=mesh, in_specs=in_specs, out_specs=tok_spec, check_vma=False)
```

```python
import functools

import jax
import jax.numpy as jnp
from jax import lax
from jax.experimental import pallas as pl
from jax.experimental.pallas import tpu as pltpu
from jax.sharding import PartitionSpec as P

ROPE_BASE = 10000.0
NORM_EPS = 1e-6
NEG = -1e30
LOG2E = 1.4426950408889634
F32 = jnp.float32
BF16 = jnp.bfloat16
MESH = pl.DeviceIdType.MESH

ROUTE = (
    ((0, 0), (1, 1), (2, 0)),
    ((1, 0), (1, 2), (3, 0)),
    ((0, 1), (2, 1), (3, 1)),
    ((0, 2), (2, 2), (3, 2)),
)
SEND_ORDER = ((1, 2), (2,), (0, 2), (1, 0))
HOME = tuple(
    tuple(next((i, q) for i in range(4) for q in range(3) if ROUTE[i][q] == (c, s)) for s in range(3))
    for c in range(4)
)
KV_SENDS = (((0, 1, 0),), ((1, 2, 0), (2, 2, 1), (0, 0, 0)), ((0, 3, 0),), ())

ROWS = 128
TOK = 3 * ROWS
TN = 1024
TH = 512
SLOTS = 5
HG = 8


def dot(a, b):
    return jnp.dot(a, b, preferred_element_type=F32)


def gelu_tanh(x):
    c0 = 0.7978845608028654
    t = jnp.tanh(x * (c0 + (c0 * 0.044715) * (x * x)))
    h = 0.5 * x
    return h + h * t


def layers_kernel(
    n_layers, d_model, ff,
    x_ref, cs_ref, ga_ref, gm_ref, wq_ref, wk_ref, wv_ref, wo_ref, wu_ref, wd_ref,
    y_ref,
    hbuf, nbuf, pbuf, rbuf, obuf, tab, mask, ring, qring,
    wsem, qsem, xs_sem, xr_sem, ts_sem, tr_sem, ps_sem, pr_sem, ns_sem, nr_sem, ks_sem, kr_sem, os_sem, or_sem,
    ys_sem, yr_sem, cred,
):
    me = lax.axis_index("seq")
    core = lax.rem(me, 2)
    chip = me // 2
    partner = {"seq": me + 1 - 2 * core}

    n_out = d_model // TN
    n_up = -(-ff // TN)
    n_col = d_model // TH
    up_tiles = 2 * n_up
    tail = ff - (n_up * TN - TH)
    k_units = ff // 256
    cuts = [0, (k_units // 3) * 256, 2 * (k_units // 3) * 256, ff]
    tiles = 2 * n_out + up_tiles + 6 * n_out
    o_rows = 4 * TN

    def on_chip(c):
        return {"seq": 2 * c + core}

    def cols(i):
        return pl.ds(pl.multiple_of(i * TN, TN), TN)

    def half(i):
        return pl.ds(pl.multiple_of(i * TH, TH), TH)

    def q_start(l, i):
        for kind, ref in enumerate((wk_ref, wv_ref, wq_ref)):
            for g in range(2):
                idx = 2 * g + kind if kind < 2 else 4 + g

                @pl.when(i == idx)
                def _(ref=ref, g=g, idx=idx):
                    heads = pl.ds(pl.multiple_of(core * 2 * HG + g * HG, HG), HG)
                    pltpu.make_async_copy(ref.at[l, :, heads, :], qring.at[idx % 2], qsem.at[idx % 2]).start()

    def q_wait(slot):
        pltpu.make_async_copy(wq_ref.at[0, :, pl.ds(0, HG), :], qring.at[slot], qsem.at[slot]).wait()

    def t_slot(l, t):
        return lax.rem(l * tiles + t, SLOTS)

    def out_copy(l, i):
        s = t_slot(l, i)
        return pltpu.make_async_copy(wo_ref.at[l, :, half(i)], ring.at[s, pl.ds(0, o_rows)], wsem.at[s])

    def up_copy(l, i):
        s = t_slot(l, 2 * n_out + i)
        return pltpu.make_async_copy(wu_ref.at[l, :, half(i)], ring.at[s, pl.ds(0, d_model)], wsem.at[s])

    def up_tail_copy(l):
        s = t_slot(l, 2 * n_out + up_tiles - 1)
        src = wu_ref.at[l, :, pl.ds((up_tiles - 1) * TH, tail)]
        return pltpu.make_async_copy(src, ring.at[s, pl.ds(0, d_model), pl.ds(0, tail)], wsem.at[s])

    def down_copy(l, n, kk, j):
        s = t_slot(l, 2 * n_out + up_tiles + 6 * n + 2 * kk + j)
        size = cuts[kk + 1] - cuts[kk]
        return pltpu.make_async_copy(
            wd_ref.at[l, pl.ds(cuts[kk], size), half(2 * n + j)], ring.at[s, pl.ds(0, size)], wsem.at[s])

    def up_start(l, i):
        @pl.when(i < up_tiles - 1)
        def _():
            up_copy(l, i).start()

        @pl.when(i == up_tiles - 1)
        def _():
            up_tail_copy(l).start()

        for d in range(3):
            @pl.when(i == up_tiles + d)
            def _(d=d):
                down_copy(l, 0, d // 2, d % 2).start()

    q_start(0, 0)
    for i in range(3):
        out_copy(0, i).start()

    barrier = pltpu.get_barrier_semaphore()
    for k in range(1, 8):
        pl.semaphore_signal(barrier, inc=1, device_id={"seq": lax.rem(me + k, 8)}, device_id_type=MESH)
    pl.semaphore_wait(barrier, 7)

    def rows(t):
        return pl.ds(t * ROWS if isinstance(t, int) else pl.multiple_of(t * ROWS, ROWS), ROWS)

    def tab_send(c, k, q):
        dst, slot = ROUTE[c][q]
        return pltpu.make_async_remote_copy(
            src_ref=cs_ref, dst_ref=tab.at[0, rows(slot)], send_sem=ts_sem.at[k],
            recv_sem=tr_sem.at[slot], device_id=on_chip(dst), device_id_type=MESH)

    def tab_pair(t):
        return pltpu.make_async_remote_copy(
            src_ref=tab.at[0, rows(t)], dst_ref=tab.at[1, rows(t)], send_sem=ps_sem.at[t],
            recv_sem=pr_sem.at[t], device_id=partner, device_id_type=MESH)

    for c in range(4):
        @pl.when(chip == c)
        def _(c=c):
            for k, q in enumerate(SEND_ORDER[c]):
                dst, slot = ROUTE[c][q]
                pltpu.make_async_remote_copy(
                    src_ref=x_ref.at[q], dst_ref=hbuf.at[rows(slot)], send_sem=xs_sem.at[k],
                    recv_sem=xr_sem.at[slot], device_id=on_chip(dst), device_id_type=MESH).start()
                tab_send(c, k, q).start()
            for q in range(3):
                dst, slot = ROUTE[c][q]
                if dst == c:
                    pltpu.make_async_copy(x_ref.at[q], hbuf.at[rows(slot)], xr_sem.at[slot]).start()
                    pltpu.make_async_copy(cs_ref, tab.at[0, rows(slot)], tr_sem.at[slot]).start()

    ri = lax.broadcasted_iota(jnp.int32, (2 * ROWS, 2 * ROWS), 0)
    ci = lax.broadcasted_iota(jnp.int32, (2 * ROWS, 2 * ROWS), 1)
    flip = core * ROWS
    rp = jnp.where(ri < ROWS, ri + flip, ri - flip)
    cp = jnp.where(ci < ROWS, ci + flip, ci - flip)
    mask[...] = jnp.where(cp <= rp, 0.0, NEG)

    def norm_rows(gain, t):
        for i in range(ROWS // 16):
            r = pl.ds(pl.multiple_of(t * ROWS + i * 16, 16), 16)
            v = hbuf[r, :].astype(F32)
            scale = lax.rsqrt(jnp.mean(v * v, axis=1, keepdims=True) + NORM_EPS)
            nbuf[0, r, :] = (v * scale * gain).astype(BF16)

    def n_send(t):
        return pltpu.make_async_remote_copy(
            src_ref=nbuf.at[0, rows(t)], dst_ref=nbuf.at[1, rows(t)], send_sem=ns_sem.at[t],
            recv_sem=nr_sem.at[t], device_id=partner, device_id_type=MESH)

    def kv_send(i, s, k, slot, dst, rslot):
        base = 4 + 4 * (i % 2) + 2 * (i // 2) if isinstance(i, int) else 4 + 4 * lax.rem(i, 2) + 2 * (i // 2)
        return pltpu.make_async_remote_copy(
            src_ref=pbuf.at[base + s, rows(slot)], dst_ref=rbuf.at[i, rslot, s], send_sem=ks_sem.at[i, s, k],
            recv_sem=kr_sem.at[i, rslot, s], device_id=on_chip(dst), device_id_type=MESH)

    def kv_wait(i, s, rslot):
        pltpu.make_async_remote_copy(
            src_ref=pbuf.at[0, rows(0)], dst_ref=rbuf.at[i, rslot, s], send_sem=ks_sem.at[i, s, 0],
            recv_sem=kr_sem.at[i, rslot, s], device_id=partner, device_id_type=MESH).wait_recv()

    def o_send(g):
        return pltpu.make_async_remote_copy(
            src_ref=pbuf.at[2 * g + 1], dst_ref=obuf.at[g], send_sem=os_sem.at[g],
            recv_sem=or_sem.at[g], device_id=partner, device_id_type=MESH)

    def layer(l, _):
        gain = ga_ref[pl.ds(l, 1), :]

        def norm_chunk(t, _):
            @pl.when(l == 0)
            def _():
                pltpu.make_async_copy(x_ref.at[0], hbuf.at[rows(t)], xr_sem.at[t]).wait()
                pltpu.make_async_copy(cs_ref, tab.at[0, rows(t)], tr_sem.at[t]).wait()
                tab_pair(t).start()

            @pl.when(t > 0)
            def _():
                n_send(t - 1).start()

            norm_rows(gain, t)
            return 0

        lax.fori_loop(0, 3, norm_chunk, 0)

        def qkv_tile(i, _):
            slot = lax.rem(i, 2)
            q_wait(slot)

            @pl.when(i < 5)
            def _():
                q_start(l, i + 1)

            @pl.when(jnp.logical_and(i == 5, l < n_layers - 1))
            def _():
                q_start(l + 1, 0)

            def side(s, _):
                b = 2 * i + s

                @pl.when(b == 0)
                def _():
                    n_send(2).start()

                @pl.when(b == 1)
                def _():
                    for t in range(3):
                        n_send(t).wait_recv()

                    @pl.when(l == 0)
                    def _():
                        for t in range(3):
                            tab_pair(t).wait()

                    @pl.when(l > 0)
                    def _():
                        for c in range(4):
                            @pl.when(chip == c)
                            def _(c=c):
                                for k in sorted({1 if dst == 2 else 0 for _, dst, _ in KV_SENDS[c]}):
                                    pl.semaphore_wait(cred.at[k], 1)

                @pl.when(jnp.logical_and(b >= 1, b <= 8))
                def _():
                    pi = (b - 1) // 2
                    ps = lax.rem(b - 1, 2)
                    for c in range(4):
                        @pl.when(chip == c)
                        def _(c=c):
                            for k, (sl, dst, rs) in enumerate(KV_SENDS[c]):
                                kv_send(pi, ps, k, sl, dst, rs).start()

                kq = d_model // 8
                u = functools.reduce(jnp.add, [
                    dot(nbuf[s, :, j * kq:(j + 1) * kq], qring[slot, j * kq:(j + 1) * kq].reshape(kq, TN))
                    for j in range(8)])
                piece = jnp.where(i < 4, 4 + 4 * lax.rem(i, 2) + 2 * (i // 2), 2 * (i - 4)) + s
                plain = jnp.logical_and(lax.rem(i, 2) == 1, i < 4)
                cs = tab[s]
                sc = pltpu.roll(cs, 64, axis=1)
                first = lax.broadcasted_iota(jnp.int32, (TOK, 128), 1) < 64
                cos = jnp.where(plain, 1.0, jnp.where(first, cs, sc))
                sin = jnp.where(plain, 0.0, jnp.where(first, -sc, cs))
                for h in range(HG):
                    uh = u[:, h * 128:(h + 1) * 128]
                    pbuf[piece, :, h * 128:(h + 1) * 128] = (
                        uh * cos + pltpu.roll(uh, 64, axis=1) * sin).astype(BF16)

                @pl.when(jnp.logical_and(i < 4, chip != 2))
                def _():
                    rbuf[jnp.minimum(i, 3), 1, s] = pbuf[piece, 0:ROWS, :]

                return 0

            lax.fori_loop(0, 2, side, 0)
            return 0

        lax.fori_loop(0, 6, qkv_tile, 0)
        for t in range(3):
            n_send(t).wait_send()

        bias0 = jnp.where(lax.rem(chip, 2) == 1, 0.0, NEG)
        bias1 = jnp.where(chip == 1, NEG, 0.0)
        c2 = 128 ** -0.5 * LOG2E

        def group(g, _):
            for j in range(2):
                for s in range(2):
                    kv_wait(2 * g + j, s, 0)

            @pl.when(chip == 2)
            def _():
                for j in range(2):
                    for s in range(2):
                        kv_wait(2 * g + j, s, 1)

            @pl.when(g == 1)
            def _():
                o_send(0).start()

            def head(h, _):
                lanes = pl.ds(pl.multiple_of(h * 128, 128), 128)

                def local(base, t):
                    r = rows(t)
                    return jnp.concatenate([pbuf[base + 2 * g, r, lanes], pbuf[base + 2 * g + 1, r, lanes]], axis=0)

                def remote(j, rs):
                    return jnp.concatenate([rbuf[2 * g + j, rs, 0, :, lanes], rbuf[2 * g + j, rs, 1, :, lanes]], axis=0)

                for t in range(3):
                    q = local(0, t)
                    blocks = [(remote(0, 0), remote(1, 0), bias0 if t == 0 else bias1)]
                    if t > 0:
                        blocks.append((remote(0, 1), remote(1, 1), bias1))
                    if t == 2:
                        blocks.append((local(4, 1), local(8, 1), None))
                    blocks.append((local(4, t), local(8, t), mask[...]))
                    xs = []
                    for k, _, b in blocks:
                        sc = lax.dot_general(q, k, (((1,), (1,)), ((), ())), preferred_element_type=F32) * c2
                        xs.append(sc if b is None else sc + b)
                    top = functools.reduce(jnp.maximum, xs)
                    top = jnp.max(top, axis=1, keepdims=True)
                    es = [jnp.exp2(v - top) for v in xs]
                    total = jnp.sum(functools.reduce(jnp.add, es), axis=1, keepdims=True)
                    o = functools.reduce(jnp.add, [dot(e.astype(BF16), v) for e, (_, v, _) in zip(es, blocks)])
                    o = (o * (1.0 / total)).astype(BF16)
                    pbuf[2 * g, rows(t), lanes] = o[:ROWS]
                    pbuf[2 * g + 1, rows(t), lanes] = o[ROWS:]
                return 0

            lax.fori_loop(0, HG, head, 0)
            return 0

        lax.fori_loop(0, 2, group, 0)

        for c in range(4):
            @pl.when(chip == c)
            def _(c=c):
                for i in range(4):
                    for s in range(2):
                        for k, (sl, dst, rs) in enumerate(KV_SENDS[c]):
                            kv_send(i, s, k, sl, dst, rs).wait_send()

                @pl.when(l < n_layers - 1)
                def _():
                    src, k = ((1, 0), (0, 0), (1, 1), (2, 0))[c]
                    pl.semaphore_signal(cred.at[k], inc=1, device_id=on_chip(src), device_id_type=MESH)

        o_send(1).start()
        for g in range(2):
            o_send(g).wait_recv()

        def out_start(i):
            @pl.when(i < 2 * n_out)
            def _():
                out_copy(l, i).start()

            @pl.when(i >= 2 * n_out)
            def _():
                up_start(l, i - 2 * n_out)

        def out_tile(i, _):
            out_copy(l, 2 * i).wait()
            out_copy(l, 2 * i + 1).wait()

            out_start(2 * i + 3)
            out_start(2 * i + 4)
            for j in range(2):
                slot = t_slot(l, 2 * i + j)
                mine = [dot(pbuf[2 * g], ring[slot, cols(2 * core + g), :]) for g in range(2)]
                other = [dot(obuf[g], ring[slot, cols(2 - 2 * core + g), :]) for g in range(2)]
                u = functools.reduce(jnp.add, mine + other)
                c = half(2 * i + j)
                hbuf[:, c] = (hbuf[:, c].astype(F32) + u).astype(BF16)
            return 0

        lax.fori_loop(0, n_out, out_tile, 0)
        for g in range(2):
            o_send(g).wait_send()

        gain_m = gm_ref[pl.ds(l, 1), :]

        def norm_mlp(t, _):
            norm_rows(gain_m, t)
            return 0

        lax.fori_loop(0, 3, norm_mlp, 0)

        def up_tile(i, _):
            up_copy(l, 2 * i).wait()

            @pl.when(i < n_up - 1)
            def _():
                up_copy(l, 2 * i + 1).wait()

            @pl.when(i == n_up - 1)
            def _():
                up_tail_copy(l).wait()

            up_start(l, 2 * i + 3)
            up_start(l, 2 * i + 4)
            for j in range(2):
                slot = t_slot(l, 2 * n_out + 2 * i + j)
                pbuf[i, :, j * TH:(j + 1) * TH] = gelu_tanh(dot(nbuf[0], ring[slot, 0:d_model, :])).astype(BF16)
            return 0

        lax.fori_loop(0, n_up, up_tile, 0)

        def y_send(c, t, n):
            dst, q = HOME[c][t]
            if dst == c:
                return pltpu.make_async_copy(hbuf.at[rows(t), half(n)], y_ref.at[q, :, half(n)], yr_sem.at[q, n])
            return pltpu.make_async_remote_copy(
                src_ref=hbuf.at[rows(t), half(n)], dst_ref=y_ref.at[q, :, half(n)], send_sem=ys_sem.at[t, n],
                recv_sem=yr_sem.at[q, n], device_id=on_chip(dst), device_id_type=MESH)

        def y_start(n):
            for c in range(4):
                @pl.when(chip == c)
                def _(c=c):
                    for t in range(3):
                        y_send(c, t, n).start()

        def down_start(n, kk, j):
            @pl.when(n < n_out)
            def _():
                down_copy(l, n, kk, j).start()

            @pl.when(jnp.logical_and(n >= n_out, l < n_layers - 1))
            def _():
                out_copy(l + 1, 2 * kk + j).start()

        def down_tile(n, _):
            total = [None, None]
            for kk in range(3):
                for j in range(2):
                    down_copy(l, n, kk, j).wait()
                down_start(n + (kk + 1) // 3, (kk + 1) % 3, 1)
                down_start(n + (kk + 2) // 3, (kk + 2) % 3, 0)
                if kk == 0:
                    @pl.when(jnp.logical_and(n > 0, l == n_layers - 1))
                    def _():
                        y_start(2 * n - 2)
                        y_start(2 * n - 1)

                for j in range(2):
                    slot = t_slot(l, 2 * n_out + up_tiles + 6 * n + 2 * kk + j)
                    parts = [] if total[j] is None else [total[j]]
                    lo = cuts[kk]
                    while lo < cuts[kk + 1]:
                        hi = min((lo // TN + 1) * TN, cuts[kk + 1])
                        parts.append(dot(pbuf[lo // TN, :, lo % TN:lo % TN + hi - lo],
                                         ring[slot, lo - cuts[kk]:hi - cuts[kk], :]))
                        lo = hi
                    total[j] = functools.reduce(jnp.add, parts)
            for j in range(2):
                c = half(2 * n + j)
                hbuf[:, c] = (hbuf[:, c].astype(F32) + total[j]).astype(BF16)
            return 0

        lax.fori_loop(0, n_out, down_tile, 0)

        @pl.when(l == n_layers - 1)
        def _():
            for c in range(4):
                @pl.when(chip == c)
                def _(c=c):
                    for k, q in enumerate(SEND_ORDER[c]):
                        dst, slot = ROUTE[c][q]
                        pltpu.make_async_remote_copy(
                            src_ref=x_ref.at[q], dst_ref=hbuf.at[rows(slot)], send_sem=xs_sem.at[k],
                            recv_sem=xr_sem.at[slot], device_id=on_chip(dst), device_id_type=MESH).wait_send()
                        tab_send(c, k, q).wait_send()
            y_start(n_col - 2)
            y_start(n_col - 1)
            for c in range(4):
                @pl.when(chip == c)
                def _(c=c):
                    for n in range(n_col):
                        for t in range(3):
                            if HOME[c][t][0] != c:
                                y_send(c, t, n).wait_send()
            for n in range(n_col):
                for q in range(3):
                    pltpu.make_async_copy(hbuf.at[rows(0), half(n)], y_ref.at[q, :, half(n)], yr_sem.at[q, n]).wait()

        return 0

    lax.fori_loop(0, n_layers, layer, 0)


def run_layers(x_loc, cs_loc, g_attn, g_mlp, w_query, w_key, w_value, w_out, w_up, w_down):
    n_layers, d_model = g_attn.shape
    ff = w_up.shape[-1]
    n_col = d_model // TH
    k_units = ff // 256
    ring_rows = max(4 * TN, d_model, (k_units - 2 * (k_units // 3)) * 256)
    vmem = pl.BlockSpec(memory_space=pltpu.VMEM)
    hbm = pl.BlockSpec(memory_space=pl.ANY)
    dma = pltpu.SemaphoreType.DMA
    n_pieces = max(12, -(-ff // TN))
    return pl.pallas_call(
        functools.partial(layers_kernel, n_layers, d_model, ff),
        out_shape=jax.ShapeDtypeStruct(x_loc.shape, BF16),
        in_specs=[hbm, hbm, vmem, vmem] + [hbm] * 6,
        out_specs=hbm,
        scratch_shapes=[
            pltpu.VMEM((TOK, d_model), BF16),
            pltpu.VMEM((2, TOK, d_model), BF16),
            pltpu.VMEM((n_pieces, TOK, TN), BF16),
            pltpu.VMEM((4, 2, 2, ROWS, TN), BF16),
            pltpu.VMEM((2, TOK, TN), BF16),
            pltpu.VMEM((2, TOK, 128), F32),
            pltpu.VMEM((2 * ROWS, 2 * ROWS), F32),
            pltpu.VMEM((SLOTS, ring_rows, TH), BF16),
            pltpu.VMEM((2, d_model, HG, 128), BF16),
            dma((SLOTS,)), dma((2,)), dma((2,)), dma((3,)), dma((2,)), dma((3,)), dma((3,)), dma((3,)),
            dma((3,)), dma((3,)), dma((4, 2, 3)), dma((4, 2, 2)), dma((2,)), dma((2,)),
            dma((3, n_col)), dma((3, n_col)),
            pltpu.SemaphoreType.REGULAR((2,)),
        ],
        compiler_params=pltpu.CompilerParams(
            collective_id=0, has_side_effects=True, vmem_limit_bytes=67043328),
        name="layers",
    )(x_loc, cs_loc, g_attn, g_mlp, w_query, w_key, w_value, w_out.reshape(n_layers, -1, d_model), w_up, w_down)


def rope_table(pos_loc):
    lane = lax.broadcasted_iota(jnp.int32, (1, 128), 1)
    inv_freq = ROPE_BASE ** (-(lane % 64).astype(F32) * (2.0 / 128))
    angles = pos_loc.astype(F32)[:, None] * inv_freq
    return jnp.where(lane < 64, jnp.cos(angles), jnp.sin(angles))


def solution(mesh):
    tok_spec = P(None, ("data", "seq"), None)
    in_specs = (tok_spec, P(("data", "seq"))) + (P(),) * 8

    def device_fn(x_loc, pos_loc, w_query, w_key, w_value, w_out, w_up, w_down, g_attn, g_mlp):
        return run_layers(x_loc, rope_table(pos_loc), g_attn, g_mlp, w_query, w_key, w_value, w_out, w_up, w_down)

    return jax.shard_map(device_fn, mesh=mesh, in_specs=in_specs, out_specs=tok_spec, check_vma=False)
```

```python
import functools

import jax
import jax.numpy as jnp
from jax import lax
from jax.experimental import pallas as pl
from jax.experimental.pallas import tpu as pltpu
from jax.sharding import PartitionSpec as P

ROPE_BASE = 10000.0
NORM_EPS = 1e-6
NEG = -1e30
LOG2E = 1.4426950408889634
F32 = jnp.float32
BF16 = jnp.bfloat16
MESH = pl.DeviceIdType.MESH

ROUTE = (
    ((0, 0), (1, 1), (2, 0)),
    ((1, 0), (1, 2), (3, 0)),
    ((0, 1), (2, 1), (3, 1)),
    ((0, 2), (2, 2), (3, 2)),
)
SEND_ORDER = ((1, 2), (2,), (0, 2), (1, 0))
HOME = tuple(
    tuple(next((i, q) for i in range(4) for q in range(3) if ROUTE[i][q] == (c, s)) for s in range(3))
    for c in range(4)
)
KV_SENDS = (((0, 1, 1),), ((1, 2, 2), (0, 1, 0)), ((0, 1, 3),), ())

ROWS = 128
TOK = 3 * ROWS
TN = 1024
TH = 512
SLOTS = 5
HG = 8


def dot(a, b):
    return jnp.dot(a, b, preferred_element_type=F32)


def gelu_tanh(x):
    c0 = 0.7978845608028654
    t = jnp.tanh(x * (c0 + (c0 * 0.044715) * (x * x)))
    h = 0.5 * x
    return h + h * t


def layers_kernel(
    n_layers, d_model, ff,
    x_ref, cs_ref, ga_ref, gm_ref, wq_ref, wk_ref, wv_ref, wo_ref, wu_ref, wd_ref,
    y_ref,
    hbuf, nbuf, pbuf, rbuf, obuf, tab, mask, ring, qring,
    wsem, qsem, xs_sem, xr_sem, ts_sem, tr_sem, ps_sem, pr_sem, ns_sem, nr_sem, ks_sem, kr_sem, kt_sem, ku_sem, os_sem, or_sem,
    ys_sem, yr_sem, cred,
):
    me = lax.axis_index("seq")
    core = lax.rem(me, 2)
    chip = me // 2
    partner = {"seq": me + 1 - 2 * core}

    n_out = d_model // TN
    n_up = -(-ff // TN)
    n_col = d_model // TH
    up_tiles = 2 * n_up
    tail = ff - (n_up * TN - TH)
    k_units = ff // 256
    cuts = [0, (k_units // 3) * 256, 2 * (k_units // 3) * 256, ff]
    tiles = 2 * n_out + up_tiles + 6 * n_out
    o_rows = 4 * TN

    def on_chip(c):
        return {"seq": 2 * c + core}

    def by_core(order, send):
        order = list(order)
        if len(order) < 2:
            send(order)
        else:
            pl.when(core == 0)(lambda: send(order))
            pl.when(core == 1)(lambda: send(order[::-1]))

    def cols(i):
        return pl.ds(pl.multiple_of(i * TN, TN), TN)

    def half(i):
        return pl.ds(pl.multiple_of(i * TH, TH), TH)

    def q_start(l, i):
        for kind, ref in enumerate((wk_ref, wv_ref, wq_ref)):
            for g in range(2):
                idx = 2 * g + kind if kind < 2 else 4 + g

                @pl.when(i == idx)
                def _(ref=ref, g=g, idx=idx):
                    heads = pl.ds(pl.multiple_of(core * 2 * HG + g * HG, HG), HG)
                    pltpu.make_async_copy(ref.at[l, :, heads, :], qring.at[idx % 2], qsem.at[idx % 2]).start()

    def q_wait(slot):
        pltpu.make_async_copy(wq_ref.at[0, :, pl.ds(0, HG), :], qring.at[slot], qsem.at[slot]).wait()

    def t_slot(l, t):
        return lax.rem(l * tiles + t, SLOTS)

    def out_copy(l, i):
        s = t_slot(l, i)
        return pltpu.make_async_copy(wo_ref.at[l, :, half(i)], ring.at[s, pl.ds(0, o_rows)], wsem.at[s])

    def up_copy(l, i):
        s = t_slot(l, 2 * n_out + i)
        return pltpu.make_async_copy(wu_ref.at[l, :, half(i)], ring.at[s, pl.ds(0, d_model)], wsem.at[s])

    def up_tail_copy(l):
        s = t_slot(l, 2 * n_out + up_tiles - 1)
        src = wu_ref.at[l, :, pl.ds((up_tiles - 1) * TH, tail)]
        return pltpu.make_async_copy(src, ring.at[s, pl.ds(0, d_model), pl.ds(0, tail)], wsem.at[s])

    def down_copy(l, n, kk, j):
        s = t_slot(l, 2 * n_out + up_tiles + 6 * n + 2 * kk + j)
        size = cuts[kk + 1] - cuts[kk]
        return pltpu.make_async_copy(
            wd_ref.at[l, pl.ds(cuts[kk], size), half(2 * n + j)], ring.at[s, pl.ds(0, size)], wsem.at[s])

    def up_start(l, i):
        @pl.when(i < up_tiles - 1)
        def _():
            up_copy(l, i).start()

        @pl.when(i == up_tiles - 1)
        def _():
            up_tail_copy(l).start()

        for d in range(3):
            @pl.when(i == up_tiles + d)
            def _(d=d):
                down_copy(l, 0, d // 2, d % 2).start()

    q_start(0, 0)
    for i in range(3):
        out_copy(0, i).start()

    barrier = pltpu.get_barrier_semaphore()
    for k in range(1, 8):
        pl.semaphore_signal(barrier, inc=1, device_id={"seq": lax.rem(me + k, 8)}, device_id_type=MESH)
    pl.semaphore_wait(barrier, 7)

    def rows(t):
        return pl.ds(t * ROWS if isinstance(t, int) else pl.multiple_of(t * ROWS, ROWS), ROWS)

    def tab_send(c, k, q):
        dst, slot = ROUTE[c][q]
        return pltpu.make_async_remote_copy(
            src_ref=cs_ref, dst_ref=tab.at[0, rows(slot)], send_sem=ts_sem.at[k],
            recv_sem=tr_sem.at[slot], device_id=on_chip(dst), device_id_type=MESH)

    def tab_pair(t):
        return pltpu.make_async_remote_copy(
            src_ref=tab.at[0, rows(t)], dst_ref=tab.at[1, rows(t)], send_sem=ps_sem.at[t],
            recv_sem=pr_sem.at[t], device_id=partner, device_id_type=MESH)

    for c in range(4):
        @pl.when(chip == c)
        def _(c=c):
            def send(order):
                for q in order:
                    k = SEND_ORDER[c].index(q)
                    dst, slot = ROUTE[c][q]
                    pltpu.make_async_remote_copy(
                        src_ref=x_ref.at[q], dst_ref=hbuf.at[rows(slot)], send_sem=xs_sem.at[k],
                        recv_sem=xr_sem.at[slot], device_id=on_chip(dst), device_id_type=MESH).start()
                    tab_send(c, k, q).start()

            if c == 2:
                by_core(SEND_ORDER[c], send)
            else:
                send(SEND_ORDER[c])
            for q in range(3):
                dst, slot = ROUTE[c][q]
                if dst == c:
                    pltpu.make_async_copy(x_ref.at[q], hbuf.at[rows(slot)], xr_sem.at[slot]).start()
                    pltpu.make_async_copy(cs_ref, tab.at[0, rows(slot)], tr_sem.at[slot]).start()

    ri = lax.broadcasted_iota(jnp.int32, (2 * ROWS, 2 * ROWS), 0)
    ci = lax.broadcasted_iota(jnp.int32, (2 * ROWS, 2 * ROWS), 1)
    flip = core * ROWS
    rp = jnp.where(ri < ROWS, ri + flip, ri - flip)
    cp = jnp.where(ci < ROWS, ci + flip, ci - flip)
    mask[...] = jnp.where(cp <= rp, 0.0, NEG)

    def norm_rows(gain, t):
        for i in range(ROWS // 16):
            r = pl.ds(pl.multiple_of(t * ROWS + i * 16, 16), 16)
            v = hbuf[r, :].astype(F32)
            scale = lax.rsqrt(jnp.mean(v * v, axis=1, keepdims=True) + NORM_EPS)
            nbuf[0, r, :] = (v * scale * gain).astype(BF16)

    def n_send(t):
        return pltpu.make_async_remote_copy(
            src_ref=nbuf.at[0, rows(t)], dst_ref=nbuf.at[1, rows(t)], send_sem=ns_sem.at[t],
            recv_sem=nr_sem.at[t], device_id=partner, device_id_type=MESH)

    def kv_send(i, s, k, slot, n, dst):
        base = 4 + 4 * lax.rem(i, 2) + 2 * (i // 2)
        return pltpu.make_async_remote_copy(
            src_ref=pbuf.at[base + s, pl.ds(slot * ROWS, n * ROWS)],
            dst_ref=rbuf.at[i, s, pl.ds(0, n * ROWS)], send_sem=ks_sem.at[i, s, k],
            recv_sem=kr_sem.at[i, s], device_id=on_chip(dst), device_id_type=MESH)

    def tail_copy(p, k, slot, n, dst):
        lanes = pl.ds(pl.multiple_of(p * 256, 256), 256)
        return pltpu.make_async_remote_copy(
            src_ref=pbuf.at[11, pl.ds(slot * ROWS, n * ROWS), lanes],
            dst_ref=rbuf.at[3, 1, pl.ds(0, n * ROWS), lanes], send_sem=kt_sem.at[k, p],
            recv_sem=ku_sem.at[p], device_id=on_chip(dst), device_id_type=MESH)

    def tail_wait(p, n):
        tail_copy(p, 0, 0, n, 0).wait_recv()

    def kv_wait(i, n, sides=(0, 1)):
        for s in sides:
            pltpu.make_async_remote_copy(
                src_ref=pbuf.at[0, pl.ds(0, n * ROWS)], dst_ref=rbuf.at[i, s, pl.ds(0, n * ROWS)],
                send_sem=ks_sem.at[i, s, 0], recv_sem=kr_sem.at[i, s], device_id=partner,
                device_id_type=MESH).wait_recv()

    def o_at(side, g):
        return (2 * side + g) * TN

    def o_send(g):
        return pltpu.make_async_remote_copy(
            src_ref=nbuf.at[0, :, pl.ds(o_at(1, g), TN)], dst_ref=obuf.at[g], send_sem=os_sem.at[g],
            recv_sem=or_sem.at[g], device_id=partner, device_id_type=MESH)

    def layer(l, _):
        gain = ga_ref[pl.ds(l, 1), :]

        def norm_chunk(t, _):
            @pl.when(l == 0)
            def _():
                pltpu.make_async_copy(x_ref.at[0], hbuf.at[rows(t)], xr_sem.at[t]).wait()
                pltpu.make_async_copy(cs_ref, tab.at[0, rows(t)], tr_sem.at[t]).wait()
                tab_pair(t).start()

            @pl.when(t > 0)
            def _():
                n_send(t - 1).start()

            norm_rows(gain, t)
            return 0

        lax.fori_loop(0, 3, norm_chunk, 0)

        def qkv_tile(i, _):
            slot = lax.rem(i, 2)
            q_wait(slot)

            @pl.when(i < 5)
            def _():
                q_start(l, i + 1)

            @pl.when(jnp.logical_and(i == 5, l < n_layers - 1))
            def _():
                q_start(l + 1, 0)

            def side(s, _):
                b = 2 * i + s

                @pl.when(b == 0)
                def _():
                    n_send(2).start()

                @pl.when(b == 1)
                def _():
                    for t in range(3):
                        n_send(t).wait_recv()

                    @pl.when(l == 0)
                    def _():
                        for t in range(3):
                            tab_pair(t).wait()

                    @pl.when(l > 0)
                    def _():
                        for c in range(4):
                            @pl.when(chip == c)
                            def _(c=c):
                                for k in sorted({1 if dst == 2 else 0 for _, _, dst in KV_SENDS[c]}):
                                    pl.semaphore_wait(cred.at[k], 1)

                @pl.when(jnp.logical_and(b >= 1, b <= 8))
                def _():
                    pi = (b - 1) // 2
                    ps = lax.rem(b - 1, 2)
                    for c in range(4):
                        @pl.when(chip == c)
                        def _(c=c):
                            def send(order):
                                for k in order:
                                    sl, n, dst = KV_SENDS[c][k]

                                    @pl.when(b < 8)
                                    def _(k=k, sl=sl, n=n, dst=dst):
                                        kv_send(pi, ps, k, sl, n, dst).start()

                                    @pl.when(b == 8)
                                    def _(k=k, sl=sl, n=n, dst=dst):
                                        for p in range(4):
                                            tail_copy(p, k, sl, n, dst).start()

                            by_core(range(len(KV_SENDS[c])), send)

                kq = d_model // 8
                u = functools.reduce(jnp.add, [
                    dot(nbuf[s, :, j * kq:(j + 1) * kq], qring[slot, j * kq:(j + 1) * kq].reshape(kq, TN))
                    for j in range(8)])
                piece = jnp.where(i < 4, 4 + 4 * lax.rem(i, 2) + 2 * (i // 2), 2 * (i - 4)) + s
                plain = jnp.logical_and(lax.rem(i, 2) == 1, i < 4)
                cs = tab[s]
                sc = pltpu.roll(cs, 64, axis=1)
                first = lax.broadcasted_iota(jnp.int32, (TOK, 128), 1) < 64
                cos = jnp.where(plain, 1.0, jnp.where(first, cs, sc))
                sin = jnp.where(plain, 0.0, jnp.where(first, -sc, cs))
                for h in range(HG):
                    uh = u[:, h * 128:(h + 1) * 128]
                    pbuf[piece, :, h * 128:(h + 1) * 128] = (
                        uh * cos + pltpu.roll(uh, 64, axis=1) * sin).astype(BF16)

                return 0

            lax.fori_loop(0, 2, side, 0)
            return 0

        lax.fori_loop(0, 6, qkv_tile, 0)
        for t in range(3):
            n_send(t).wait_send()

        c2 = 128 ** -0.5 * LOG2E

        def attend(g, h, t, others):
            lanes = pl.ds(pl.multiple_of(h * 128, 128), 128)

            def local(base, u):
                return [pbuf[base + 2 * g + s, rows(u), lanes] for s in range(2)]

            def block(j, u):
                if isinstance(u, str):
                    return jnp.concatenate([rbuf[2 * g + j, s, rows(int(u[1])), lanes] for s in range(2)], axis=0)
                return jnp.concatenate(local(4 + 4 * j, u), axis=0)

            def score(q, k):
                return lax.dot_general(q, k, (((1,), (1,)), ((), ())), preferred_element_type=F32) * c2

            q = jnp.concatenate(local(0, t), axis=0)
            slots = list(others) + [t]
            xs = [lax.dot_general(q, block(0, u), (((1,), (1,)), ((), ())), preferred_element_type=F32) * c2 for u in slots]
            xs[-1] = xs[-1] + mask[...]
            top = jnp.max(functools.reduce(jnp.maximum, xs), axis=1, keepdims=True)
            es = [jnp.exp2(x - top) for x in xs]
            total = jnp.sum(functools.reduce(jnp.add, es), axis=1, keepdims=True)
            o = functools.reduce(jnp.add, [dot(e.astype(BF16), block(1, u)) for e, u in zip(es, slots)])
            o = (o * (1.0 / total)).astype(BF16)
            for s in range(2):
                nbuf[0, rows(t), pl.ds(pl.multiple_of(o_at(s, g) + h * 128, 128), 128)] = o[s * ROWS:(s + 1) * ROWS]

        def group_wait(g, n):
            kv_wait(2 * g, n)
            kv_wait(2 * g + 1, n, (0,))

            @pl.when(g == 0)
            def _():
                kv_wait(1, n, (1,))

        def heads(g, work, n=None):
            def step(h, c):
                if n is not None:
                    @pl.when(jnp.logical_and(g == 1, lax.rem(h, 2) == 0))
                    def _():
                        tail_wait(h // 2, n)

                for t, others in work[::-1]:
                    attend(g, h, t, others)
                return c

            lax.fori_loop(0, HG, step, 0)

        def groups(n, work):
            def step(g, c):
                group_wait(g, n)

                @pl.when(g == 1)
                def _():
                    o_send(0).start()

                heads(g, work, n)
                return c

            lax.fori_loop(0, 2, step, 0)

        @pl.when(chip == 0)
        def _():
            groups(1, ((0, ()), (1, ("r0", 0)), (2, ("r0", 0, 1))))

        @pl.when(chip == 1)
        def _():
            def first_step(g, c):
                heads(g, ((1, ()), (2, (1,))))
                return c

            lax.fori_loop(0, 2, first_step, 0)

            def last_step(g, c):
                group_wait(g, 1)

                @pl.when(g == 1)
                def _():
                    o_send(0).start()

                heads(g, ((0, ("r0",)),), 1)
                return c

            lax.fori_loop(0, 2, last_step, 0)

        @pl.when(chip == 2)
        def _():
            groups(2, ((0, ()), (1, ("r0", "r1")), (2, ("r0", "r1", 1))))

        @pl.when(chip == 3)
        def _():
            groups(1, ((0, ("r0",)), (1, ("r0", 0)), (2, ("r0", 0, 1))))

        for c in range(4):
            @pl.when(chip == c)
            def _(c=c):
                for k, (sl, n, dst) in enumerate(KV_SENDS[c]):
                    for i in range(4):
                        for s in range(2 if i < 3 else 1):
                            kv_send(i, s, k, sl, n, dst).wait_send()
                    for p in range(4):
                        tail_copy(p, k, sl, n, dst).wait_send()

                @pl.when(l < n_layers - 1)
                def _():
                    src, k = ((1, 0), (0, 0), (1, 1), (2, 0))[c]
                    pl.semaphore_signal(cred.at[k], inc=1, device_id=on_chip(src), device_id_type=MESH)

        o_send(1).start()

        def out_start(i):
            @pl.when(i < 2 * n_out)
            def _():
                out_copy(l, i).start()

            @pl.when(i >= 2 * n_out)
            def _():
                up_start(l, i - 2 * n_out)

        def out_tile(i, _):
            out_copy(l, 2 * i).wait()
            out_copy(l, 2 * i + 1).wait()

            out_start(2 * i + 3)
            out_start(2 * i + 4)
            slots = [t_slot(l, 2 * i + j) for j in range(2)]
            us = [functools.reduce(jnp.add, [dot(nbuf[0, :, o_at(0, g):o_at(0, g) + TN], ring[slot, cols(2 * core + g), :]) for g in range(2)])
                  for slot in slots]

            @pl.when(i == 0)
            def _():
                for g in range(2):
                    o_send(g).wait_recv()

            for j, slot in enumerate(slots):
                other = [dot(obuf[g], ring[slot, cols(2 - 2 * core + g), :]) for g in range(2)]
                c = half(2 * i + j)
                hbuf[:, c] = (hbuf[:, c].astype(F32) + (us[j] + functools.reduce(jnp.add, other))).astype(BF16)
            return 0

        lax.fori_loop(0, n_out, out_tile, 0)
        for g in range(2):
            o_send(g).wait_send()

        gain_m = gm_ref[pl.ds(l, 1), :]

        def norm_mlp(t, _):
            norm_rows(gain_m, t)
            return 0

        lax.fori_loop(0, 3, norm_mlp, 0)

        def up_tile(i, _):
            up_copy(l, 2 * i).wait()

            @pl.when(i < n_up - 1)
            def _():
                up_copy(l, 2 * i + 1).wait()

            @pl.when(i == n_up - 1)
            def _():
                up_tail_copy(l).wait()

            up_start(l, 2 * i + 3)
            up_start(l, 2 * i + 4)
            for j in range(2):
                slot = t_slot(l, 2 * n_out + 2 * i + j)
                pbuf[i, :, j * TH:(j + 1) * TH] = gelu_tanh(dot(nbuf[0], ring[slot, 0:d_model, :])).astype(BF16)
            return 0

        lax.fori_loop(0, n_up, up_tile, 0)

        def y_send(c, t, n):
            dst, q = HOME[c][t]
            if dst == c:
                return pltpu.make_async_copy(hbuf.at[rows(t), half(n)], y_ref.at[q, :, half(n)], yr_sem.at[q, n])
            return pltpu.make_async_remote_copy(
                src_ref=hbuf.at[rows(t), half(n)], dst_ref=y_ref.at[q, :, half(n)], send_sem=ys_sem.at[t, n],
                recv_sem=yr_sem.at[q, n], device_id=on_chip(dst), device_id_type=MESH)

        def y_start(n):
            for c in range(4):
                @pl.when(chip == c)
                def _(c=c):
                    def send(order):
                        for t in order:
                            y_send(c, t, n).start()

                    if c == 2:
                        by_core((0, 2), send)
                        send((1,))
                    else:
                        send(range(3))

        def down_start(n, kk, j):
            @pl.when(n < n_out)
            def _():
                down_copy(l, n, kk, j).start()

            @pl.when(jnp.logical_and(n >= n_out, l < n_layers - 1))
            def _():
                out_copy(l + 1, 2 * kk + j).start()

        def down_tile(n, _):
            total = [None, None]
            for kk in range(3):
                for j in range(2):
                    down_copy(l, n, kk, j).wait()
                down_start(n + (kk + 1) // 3, (kk + 1) % 3, 1)
                down_start(n + (kk + 2) // 3, (kk + 2) % 3, 0)
                if kk == 0:
                    @pl.when(jnp.logical_and(n > 0, l == n_layers - 1))
                    def _():
                        y_start(2 * n - 2)
                        y_start(2 * n - 1)

                for j in range(2):
                    slot = t_slot(l, 2 * n_out + up_tiles + 6 * n + 2 * kk + j)
                    parts = [] if total[j] is None else [total[j]]
                    lo = cuts[kk]
                    while lo < cuts[kk + 1]:
                        hi = min((lo // TN + 1) * TN, cuts[kk + 1])
                        parts.append(dot(pbuf[lo // TN, :, lo % TN:lo % TN + hi - lo],
                                         ring[slot, lo - cuts[kk]:hi - cuts[kk], :]))
                        lo = hi
                    total[j] = functools.reduce(jnp.add, parts)
            for j in range(2):
                c = half(2 * n + j)
                hbuf[:, c] = (hbuf[:, c].astype(F32) + total[j]).astype(BF16)
            return 0

        lax.fori_loop(0, n_out, down_tile, 0)

        @pl.when(l == n_layers - 1)
        def _():
            for c in range(4):
                @pl.when(chip == c)
                def _(c=c):
                    for k, q in enumerate(SEND_ORDER[c]):
                        dst, slot = ROUTE[c][q]
                        pltpu.make_async_remote_copy(
                            src_ref=x_ref.at[q], dst_ref=hbuf.at[rows(slot)], send_sem=xs_sem.at[k],
                            recv_sem=xr_sem.at[slot], device_id=on_chip(dst), device_id_type=MESH).wait_send()
                        tab_send(c, k, q).wait_send()
            y_start(n_col - 2)
            y_start(n_col - 1)
            for c in range(4):
                @pl.when(chip == c)
                def _(c=c):
                    for n in range(n_col):
                        for t in range(3):
                            if HOME[c][t][0] != c:
                                y_send(c, t, n).wait_send()
            for n in range(n_col):
                for q in range(3):
                    pltpu.make_async_copy(hbuf.at[rows(0), half(n)], y_ref.at[q, :, half(n)], yr_sem.at[q, n]).wait()

        return 0

    lax.fori_loop(0, n_layers, layer, 0)


def run_layers(x_loc, cs_loc, g_attn, g_mlp, w_query, w_key, w_value, w_out, w_up, w_down):
    n_layers, d_model = g_attn.shape
    ff = w_up.shape[-1]
    n_col = d_model // TH
    k_units = ff // 256
    ring_rows = max(4 * TN, d_model, (k_units - 2 * (k_units // 3)) * 256)
    vmem = pl.BlockSpec(memory_space=pltpu.VMEM)
    hbm = pl.BlockSpec(memory_space=pl.ANY)
    dma = pltpu.SemaphoreType.DMA
    n_pieces = max(12, -(-ff // TN))
    return pl.pallas_call(
        functools.partial(layers_kernel, n_layers, d_model, ff),
        out_shape=jax.ShapeDtypeStruct(x_loc.shape, BF16),
        in_specs=[hbm, hbm, vmem, vmem] + [hbm] * 6,
        out_specs=hbm,
        scratch_shapes=[
            pltpu.VMEM((TOK, d_model), BF16),
            pltpu.VMEM((2, TOK, d_model), BF16),
            pltpu.VMEM((n_pieces, TOK, TN), BF16),
            pltpu.VMEM((4, 2, 2 * ROWS, TN), BF16),
            pltpu.VMEM((2, TOK, TN), BF16),
            pltpu.VMEM((2, TOK, 128), F32),
            pltpu.VMEM((2 * ROWS, 2 * ROWS), F32),
            pltpu.VMEM((SLOTS, ring_rows, TH), BF16),
            pltpu.VMEM((2, d_model, HG, 128), BF16),
            dma((SLOTS,)), dma((2,)), dma((2,)), dma((3,)), dma((2,)), dma((3,)), dma((3,)), dma((3,)),
            dma((3,)), dma((3,)), dma((4, 2, 2)), dma((4, 2)), dma((2, 4)), dma((4,)), dma((2,)), dma((2,)),
            dma((3, n_col)), dma((3, n_col)),
            pltpu.SemaphoreType.REGULAR((2,)),
        ],
        compiler_params=pltpu.CompilerParams(
            collective_id=0, has_side_effects=True, vmem_limit_bytes=67043328),
        name="layers",
    )(x_loc, cs_loc, g_attn, g_mlp, w_query, w_key, w_value, w_out.reshape(n_layers, -1, d_model), w_up, w_down)


def rope_table(pos_loc):
    lane = lax.broadcasted_iota(jnp.int32, (1, 128), 1)
    inv_freq = ROPE_BASE ** (-(lane % 64).astype(F32) * (2.0 / 128))
    angles = pos_loc.astype(F32)[:, None] * inv_freq
    return jnp.where(lane < 64, jnp.cos(angles), jnp.sin(angles))


def solution(mesh):
    tok_spec = P(None, ("data", "seq"), None)
    in_specs = (tok_spec, P(("data", "seq"))) + (P(),) * 8

    def device_fn(x_loc, pos_loc, w_query, w_key, w_value, w_out, w_up, w_down, g_attn, g_mlp):
        return run_layers(x_loc, rope_table(pos_loc), g_attn, g_mlp, w_query, w_key, w_value, w_out, w_up, w_down)

    return jax.shard_map(device_fn, mesh=mesh, in_specs=in_specs, out_specs=tok_spec, check_vma=False)
```
